128 devices in a mesh: expert: 64 (over z, y, x_lo, core), dp: 2 (over x_hi).
Axes of the slice: x: 4 (x_hi: 2, x_lo: 2; x = x_hi * 2 + x_lo), y: 4, z: 4, core: 2. Of those that a mesh axis runs over, the one named last changes fastest.
Arguments:
- tokens: bfloat16 [16384, 2880], P(('expert', 'dp')), may hold values from -6 to 6
- cotangent: bfloat16 [16384, 2880], P(('expert', 'dp')), may hold values from -3 to 3
- expert_ids: int32 [16384, 4], P(('expert', 'dp')), may hold values from 0 to 63, as said below
- slots: int32 [16384, 4], P(('expert', 'dp')), may hold values from -1 to 5, as said below
- probs: float32 [16384, 4], P(('expert', 'dp')), may hold values from 0.1 to 0.6
- w_gate: bfloat16 [64, 2880, 1440], P('expert', None, 'dp'), may hold values from -0.109375 to 0.109375
- w_up: bfloat16 [64, 2880, 1440], P('expert', None, 'dp'), may hold values from -0.109375 to 0.109375
- w_down: bfloat16 [64, 2880, 1440], P('expert', None, 'dp'), may hold values from -0.15625 to 0.15625
Outputs:
- input_grad: bfloat16 [16384, 2880], P(('expert', 'dp'))
- prob_grad: float32 [16384, 4], P(('expert', 'dp'))
- grad_gate: bfloat16 [64, 2880, 1440], P('expert', None, 'dp')
- grad_up: bfloat16 [64, 2880, 1440], P('expert', None, 'dp')
- grad_down: bfloat16 [64, 2880, 1440], P('expert', None, 'dp')
The draws below stay inside these ranges and needn't reach their ends.
Inputs may be any that keep to these rules, and one draw needn't show every extreme that they name: `expert_ids`: each row names 4 different experts. Within the 128 tokens of one device, the choices of one expert, taken in order of tokens and then of k, hold 0, 1, 2 and so on up to 5, and -1 after that; in every draw some expert fills all 6 slots from every device.
All inputs are finite; a program needn't handle non-finite values.
Results may differ from the reference program's by a relative error of at most 0.018.
Values may be sent and summed in bfloat16 or wider, within the bound.
No kernel may reach another device: no remote copies, remote signals or barrier semaphores. Data moves between devices by JAX's collectives and lax.ppermute only.
A program may use at most 192 MiB of HBM per device.

```python
import jax
import jax.numpy as jnp
from jax import lax

D = 2880
FFW = 1440
TOP = 4
TOK_DEV = 128
EXPERTS = 64
CAP = 6
TOKENS = 16384
N_EXPERT = 64
N_DP = 2


def routing_pair(key):
    base = jax.random.fold_in(key, 11)
    first_key, second_key, third_key = jax.random.split(base, 3)
    tokens_total = TOK_DEV * N_EXPERT * N_DP
    bias = jax.random.randint(first_key, (EXPERTS,), 0, 8192)
    hottest = jax.random.randint(second_key, (), 0, EXPERTS)
    expert_range = jnp.arange(EXPERTS, dtype=jnp.int32)
    bias = bias + jnp.where(expert_range == hottest, 40000, 0)
    scores = jax.random.randint(third_key, (tokens_total, EXPERTS), 0, 65536) + bias[None, :]
    scores = scores * EXPERTS + expert_range[None, :]
    ignored, chosen = lax.top_k(scores, TOP)
    chosen = chosen.astype(jnp.int32)
    onehot = (chosen[:, :, None] == expert_range[None, None, :]).astype(jnp.int32)
    onehot = onehot.reshape(tokens_total // TOK_DEV, TOK_DEV * TOP, EXPERTS)
    ranks = jnp.cumsum(onehot, axis=1) - 1
    ranks = jnp.sum(onehot * ranks, axis=2).reshape(tokens_total, TOP)
    slot_values = jnp.where(ranks < CAP, ranks, -1).astype(jnp.int32)
    return (chosen, slot_values)


def draw_expert_ids(key, part):
    chosen, slot_values = routing_pair(key)
    return chosen


def draw_slots(key, part):
    chosen, slot_values = routing_pair(key)
    return slot_values


def block_levels(stream_key, extent, cuts, low, top_value):
    loudness, own = 1.0, jax.random.fold_in(stream_key, 6)
    for dim, parts in cuts:
        steps = jnp.exp(jax.random.uniform(jax.random.fold_in(own, dim), (parts,), jnp.float32, low / len(cuts), top_value / len(cuts)))
        loudness = loudness * jnp.repeat(steps, extent[dim] // parts).reshape([-1 if axis == dim else 1 for axis in range(len(extent))])
    return loudness


def noise(rng, shape, width, most, cuts=(), held_as=jnp.bfloat16):
    drawn = width * jax.random.normal(rng, shape, jnp.float32)
    if cuts:
        drawn = drawn * block_levels(rng, shape, cuts, -0.22, 0.18)
    return jnp.clip(drawn, -most, most).astype(held_as)


def setup_inputs(seed: int = 0) -> dict:
    streams_of = jax.random.split(jax.random.key(seed), 9)
    return {
        "tokens": noise(streams_of[0], (TOKENS, D), 1.0, 6.0, ((0, 128),)),
        "cotangent": noise(streams_of[1], (TOKENS, D), 0.4, 3.0, ((0, 128),)),
        "expert_ids": draw_expert_ids(jax.random.fold_in(streams_of[8], 71), 0),
        "slots": draw_slots(jax.random.fold_in(streams_of[8], 71), 0),
        "probs": jnp.clip(0.1 + 0.5 * jax.random.uniform(streams_of[4], (TOKENS, TOP), jnp.float32) ** block_levels(streams_of[4], (TOKENS, TOP), ((0, 128),), -0.2, 0.2), 0.1, 0.6),
        "w_gate": noise(streams_of[5], (EXPERTS, D, FFW), D ** -0.5, 0.109375, ((0, 64), (2, 2))),
        "w_up": noise(streams_of[6], (EXPERTS, D, FFW), D ** -0.5, 0.109375, ((0, 64), (2, 2))),
        "w_down": noise(streams_of[7], (EXPERTS, D, FFW), FFW ** -0.5, 0.15625, ((0, 64), (2, 2))),
    }


ALPHA = 1.702


def reference(tokens, cotangent, expert_ids, slots, probs, w_gate, w_up, w_down):
    tokens_total = tokens.shape[0]
    blocks = tokens_total // TOK_DEV
    block_of = jnp.arange(tokens_total, dtype=jnp.int32) // TOK_DEV
    kept = slots >= 0
    position = jnp.where(kept, (expert_ids * blocks + block_of[:, None]) * CAP + slots, EXPERTS * blocks * CAP)
    owners = jnp.broadcast_to(jnp.arange(tokens_total, dtype=jnp.int32)[:, None], expert_ids.shape)
    slot_owner = jnp.full((EXPERTS * blocks * CAP,), -1, jnp.int32).at[position.reshape(-1)].set(owners.reshape(-1), mode="drop")
    slot_prob = jnp.zeros((EXPERTS * blocks * CAP,), jnp.float32).at[position.reshape(-1)].set(probs.reshape(-1), mode="drop")
    slot_owner = slot_owner.reshape(EXPERTS, blocks * CAP)
    slot_prob = slot_prob.reshape(EXPERTS, blocks * CAP)

    def expert_pass(operands):
        owner_col, prob_col, gate_w, up_w, down_w = operands
        present = owner_col >= 0
        source = jnp.maximum(owner_col, 0)
        rows = jnp.where(present[:, None], tokens[source], jnp.zeros((), jnp.bfloat16))
        gate_pre = jnp.dot(rows, gate_w, preferred_element_type=jnp.float32)
        up_pre = jnp.dot(rows, up_w, preferred_element_type=jnp.float32)
        sigmoid_val = jax.nn.sigmoid(ALPHA * gate_pre)
        glu_value = gate_pre * sigmoid_val
        hidden = ((up_pre + 1.0) * glu_value).astype(jnp.bfloat16)
        outputs = lax.dot_general(hidden, down_w, (((1,), (1,)), ((), ())), preferred_element_type=jnp.float32).astype(jnp.bfloat16)
        plain = jnp.where(present[:, None], cotangent[source], jnp.zeros((), jnp.bfloat16))
        slot_grad = jnp.sum(plain.astype(jnp.float32) * outputs.astype(jnp.float32), axis=1)
        weighted = (prob_col[:, None] * plain.astype(jnp.float32)).astype(jnp.bfloat16)
        hidden_grad = jnp.dot(weighted, down_w, preferred_element_type=jnp.float32)
        up_grad = (hidden_grad * glu_value).astype(jnp.bfloat16)
        gate_grad = (hidden_grad * (up_pre + 1.0) * (sigmoid_val + ALPHA * gate_pre * sigmoid_val * (1.0 - sigmoid_val))).astype(jnp.bfloat16)
        contract_rows = (((0,), (0,)), ((), ()))
        grad_down = lax.dot_general(weighted, hidden, contract_rows, preferred_element_type=jnp.float32).astype(jnp.bfloat16)
        grad_gate = lax.dot_general(rows, gate_grad, contract_rows, preferred_element_type=jnp.float32).astype(jnp.bfloat16)
        grad_up = lax.dot_general(rows, up_grad, contract_rows, preferred_element_type=jnp.float32).astype(jnp.bfloat16)
        contract_units = (((1,), (1,)), ((), ()))
        row_grad = lax.dot_general(gate_grad, gate_w, contract_units, preferred_element_type=jnp.float32)
        row_grad = row_grad + lax.dot_general(up_grad, up_w, contract_units, preferred_element_type=jnp.float32)
        return slot_grad, row_grad.astype(jnp.bfloat16), grad_gate, grad_up, grad_down

    slot_grads, row_grads, grad_gate, grad_up, grad_down = lax.map(expert_pass, (slot_owner, slot_prob, w_gate, w_up, w_down))
    lookup = jnp.where(kept, (expert_ids * blocks + block_of[:, None]) * CAP + slots, 0)
    prob_grad = jnp.where(kept, slot_grads.reshape(-1)[lookup], jnp.float32(0.0))
    flat_rows = row_grads.reshape(-1, tokens.shape[1])
    total = jnp.zeros(tokens.shape, jnp.float32)
    for choice_index in range(TOP):
        picked = flat_rows[lookup[:, choice_index]].astype(jnp.float32)
        total = total + jnp.where(kept[:, choice_index][:, None], picked, jnp.float32(0.0))
    input_grad = total.astype(jnp.bfloat16)
    return input_grad, prob_grad, grad_gate, grad_up, grad_down
```

```python
import functools

import jax
import jax.numpy as jnp
from jax import lax
from jax.experimental import pallas as pl
from jax.experimental.pallas import tpu as pltpu
from jax.sharding import PartitionSpec as P


ALPHA = 1.702
CHUNKS = 4
GROUP = 8
HALVES = 2
PIECES = 4
BF = jnp.bfloat16
F32 = jnp.float32
NT = (((1,), (1,)), ((), ()))
NN = (((1,), (0,)), ((), ()))
TN = (((0,), (0,)), ((), ()))
ANY = pl.BlockSpec(memory_space=pl.ANY)
VMEM = pl.BlockSpec(memory_space=pltpu.VMEM)
PARAMS = pltpu.CompilerParams(vmem_limit_bytes=60 * 1024 * 1024)


def unpermute_group(recv, pick, rows_ref, b, part, width):
    size = pick.shape[0]
    lane_rows = size // CHUNKS
    blk = recv[pl.ds(pl.multiple_of(b * size, size), size), :]
    out = lax.dot_general(pick, blk, NN, preferred_element_type=F32).astype(BF)
    at = pl.ds(pl.multiple_of(b * lane_rows, lane_rows), lane_rows)
    for c in range(CHUNKS):
        w = min(part, width - c * part)
        rows_ref[at, c * part : c * part + w] = out[c * lane_rows : (c + 1) * lane_rows, :w]


def gate_up_kernel(part, recv, order, wg, wu, rows_ref, hidden, glu, slope):
    width = wg.shape[1]
    m = rows_ref.shape[0] // HALVES
    pick = order[...]

    def sort(b, carry):
        unpermute_group(recv, pick, rows_ref, b, part, width)
        return carry

    lax.fori_loop(0, recv.shape[0] // order.shape[0], sort, 0, unroll=2)

    def step(i, carry):
        at = pl.ds(pl.multiple_of(i * m, m), m)
        rows = rows_ref[at, :]
        g = lax.dot_general(rows, wg[...], NT, preferred_element_type=F32)
        u = lax.dot_general(rows, wu[...], NT, preferred_element_type=F32) + 1.0
        s = jax.nn.sigmoid(ALPHA * g)
        gl = g * s
        hidden[at, :] = (u * gl).astype(BF)
        glu[at, :] = gl
        slope[at, :] = u * (s + ALPHA * g * s * (1.0 - s))
        return carry

    lax.fori_loop(0, HALVES, step, 0)


def gate_up(recv, order, wg, wu):
    units, width = wg.shape
    total, part = recv.shape[0] // CHUNKS, recv.shape[1]
    like = jax.ShapeDtypeStruct
    return pl.pallas_call(
        functools.partial(gate_up_kernel, part),
        out_shape=(
            like((total, width), BF),
            like((total, units), BF),
            like((total, units), F32),
            like((total, units), F32),
        ),
        in_specs=[VMEM] * 4,
        out_specs=(VMEM,) * 4,
        compiler_params=PARAMS,
        name="gate_up",
    )(recv, order, wg, wu)


def row_back_kernel(
    part, recv_hbm, order, order_t, wd_hbm, wg_hbm, wu_hbm, hidden_hbm, glu_hbm, slope_hbm,
    ret_hbm, rows_hbm, gate_hbm, up_hbm,
    recv, wd, wg, wu, hidden, glu, slope, rows, gate_grad, up_grad, wide, in_sems, piece_sems, out_sems,
):
    width = wg.shape[1]
    total = rows.shape[0]
    m = total // HALVES
    last = width - (CHUNKS - 1) * part
    mark = -(-last // 128) * 128
    size = order.shape[0]
    lane_rows = size // CHUNKS
    groups = recv.shape[0] // size
    span = recv.shape[0] // PIECES

    def piece(p):
        at = pl.ds(p * span, span)
        return pltpu.make_async_copy(recv_hbm.at[at], recv.at[at], piece_sems.at[p])

    pairs = [(wd_hbm, wd), (hidden_hbm, hidden), (glu_hbm, glu), (slope_hbm, slope), (wg_hbm, wg), (wu_hbm, wu)]
    loads = [pltpu.make_async_copy(src, dst, in_sems.at[i]) for i, (src, dst) in enumerate(pairs)]
    for p in range(PIECES):
        piece(p).start()
    for load in loads:
        load.start()
    pick = order[...]
    for p in range(PIECES):
        piece(p).wait()

        def step(b, carry):
            unpermute_group(recv, pick, rows, b, part, width)
            return carry

        lax.fori_loop(p * groups // PIECES, (p + 1) * groups // PIECES, step, 0, unroll=2)
    stores = [pltpu.make_async_copy(rows, rows_hbm, out_sems.at[0])]
    stores[0].start()
    pick_t = order_t[...]
    for i in range(HALVES):
        at = pl.ds(i * m, m)
        if i == 0:
            loads[0].wait()
        hg = lax.dot_general(rows[at, :], wd[...], NT, preferred_element_type=F32)
        if i == 0:
            for load in loads[1:4]:
                load.wait()
        sg = jnp.sum(hg * hidden[at, :].astype(F32), axis=1, keepdims=True)
        ug = (hg * glu[at, :]).astype(BF)
        gg = (hg * slope[at, :]).astype(BF)
        gate_grad[at, :] = gg
        up_grad[at, :] = ug
        for j, (src, dst) in enumerate(((gate_grad, gate_hbm), (up_grad, up_hbm))):
            stores.append(pltpu.make_async_copy(src.at[at], dst.at[at], out_sems.at[1 + 3 * i + j]))
            stores[-1].start()
        low = sg - sg.astype(BF).astype(F32)
        lane = lax.broadcasted_iota(jnp.int32, (m, part - mark), 1)
        tail = jnp.where(lane == 0, sg, jnp.where(lane == 1, low, 0.0)).astype(BF)
        if last < mark:
            wide[CHUNKS - 1, :, mark - 128 : mark] = jnp.zeros((m, 128), BF)
        wide[CHUNKS - 1, :, mark:] = tail
        if i == 0:
            for load in loads[4:]:
                load.wait()
        for c in range(CHUNKS):
            w = min(part, width - c * part)
            x = lax.dot_general(gg, wg[:, c * part : c * part + w], NN, preferred_element_type=F32)
            x = x + lax.dot_general(ug, wu[:, c * part : c * part + w], NN, preferred_element_type=F32)
            wide[c, :, :w] = x.astype(BF)

        def put(b, carry):
            src = pl.ds(pl.multiple_of(b * lane_rows, lane_rows), lane_rows)
            blk = jnp.concatenate([wide[c, src, :] for c in range(CHUNKS)], axis=0)
            out = lax.dot_general(pick_t, blk, NN, preferred_element_type=F32)
            dst = pl.ds(pl.multiple_of(i * (groups // HALVES) * size + b * size, size), size)
            recv[dst, :] = out.astype(BF)
            return carry

        lax.fori_loop(0, groups // HALVES, put, 0, unroll=2)
        half = pl.ds(i * (recv.shape[0] // HALVES), recv.shape[0] // HALVES)
        stores.append(pltpu.make_async_copy(recv.at[half], ret_hbm.at[half], out_sems.at[3 + 3 * i]))
        stores[-1].start()
    for store in stores:
        store.wait()


def row_back(recv, order, order_t, wd, wg, wu, hidden, glu, slope):
    units, width = wg.shape
    total, part = recv.shape[0] // CHUNKS, recv.shape[1]
    like = jax.ShapeDtypeStruct
    return pl.pallas_call(
        functools.partial(row_back_kernel, part),
        out_shape=(like(recv.shape, BF), like((total, width), BF), like((total, units), BF), like((total, units), BF)),
        in_specs=[ANY, VMEM, VMEM] + [ANY] * 6,
        out_specs=(ANY,) * 4,
        scratch_shapes=[
            pltpu.VMEM(recv.shape, BF),
            pltpu.VMEM((units, width), BF),
            pltpu.VMEM((units, width), BF),
            pltpu.VMEM((units, width), BF),
            pltpu.VMEM((total, units), BF),
            pltpu.VMEM((total, units), F32),
            pltpu.VMEM((total, units), F32),
            pltpu.VMEM((total, width), BF),
            pltpu.VMEM((total, units), BF),
            pltpu.VMEM((total, units), BF),
            pltpu.VMEM((CHUNKS, total // HALVES, part), BF),
            pltpu.SemaphoreType.DMA((6,)),
            pltpu.SemaphoreType.DMA((PIECES,)),
            pltpu.SemaphoreType.DMA((1 + 3 * HALVES,)),
        ],
        compiler_params=PARAMS,
        name="row_back",
    )(recv, order, order_t, wd, wg, wu, hidden, glu, slope)


def combine_kernel(part, width, back, hits, masks, probs, input_grad, prob_grad, acc, pacc):
    step = pl.program_id(0)
    tops, tok = probs.shape
    last = width - (CHUNKS - 1) * part
    mark = -(-last // 128) * 128

    @pl.when(step == 0)
    def _():
        acc[...] = jnp.zeros_like(acc)
        pacc[...] = jnp.zeros_like(pacc)

    hit = hits[...]
    own = hit[:tok]
    for k in range(1, tops):
        own = own + hit[k * tok : (k + 1) * tok]
    mask = masks[...]
    spread = jnp.concatenate([own * mask[c : c + 1] for c in range(CHUNKS)], axis=0)
    blk = back[...]
    acc[...] += lax.dot_general(spread, blk, NN, preferred_element_type=F32)
    pacc[...] += lax.dot_general(hit * mask[CHUNKS - 1 : CHUNKS], blk[:, mark : mark + 128], NN, preferred_element_type=F32)

    @pl.when(step == pl.num_programs(0) - 1)
    def _():
        for c in range(CHUNKS):
            w = min(part, width - c * part)
            input_grad[c * part : c * part + w, :] = acc[c * tok : (c + 1) * tok, :].T[:w].astype(BF)
        for k in range(tops):
            col = pacc[k * tok : (k + 1) * tok, :].T
            prob_grad[k : k + 1, :] = (col[0:1] + col[1:2]) / probs[k : k + 1, :]


def combine(back, hits, masks, probs_t, width):
    rows, part = back.shape
    tops, tok = probs_t.shape
    span = masks.shape[1]
    turns = hits.shape[1] // span
    like = jax.ShapeDtypeStruct
    return pl.pallas_call(
        functools.partial(combine_kernel, part, width),
        grid=(rows // span,),
        out_shape=(like((width, tok), BF), like((tops, tok), F32)),
        in_specs=[
            pl.BlockSpec((span, part), lambda i: (i, 0)),
            pl.BlockSpec((tops * tok, span), lambda i: (0, i % turns)),
            pl.BlockSpec((CHUNKS, span), lambda i: (0, 0)),
            pl.BlockSpec((tops, tok), lambda i: (0, 0)),
        ],
        out_specs=(pl.BlockSpec((width, tok), lambda i: (0, 0)), pl.BlockSpec((tops, tok), lambda i: (0, 0))),
        scratch_shapes=[pltpu.VMEM((CHUNKS * tok, part), F32), pltpu.VMEM((tops * tok, 128), F32)],
        compiler_params=pltpu.CompilerParams(vmem_limit_bytes=24 * 1024 * 1024),
        name="combine",
    )(back, hits, masks, probs_t)


def divide(x, by):
    return jnp.floor((x.astype(F32) + 0.5) * (1.0 / by)).astype(jnp.int32)


def build_kernel(weigh, part, capacity, rows_t, position, probs, out, wide):
    width, tok = rows_t.shape
    tops = position.shape[0]

    @pl.when(pl.program_id(0) == 0)
    def _():
        wide[:width] = rows_t[...]
        wide[width:] = jnp.zeros((wide.shape[0] - width, tok), BF)

    n = out.shape[1]
    row = pl.program_id(0) * n + lax.broadcasted_iota(jnp.int32, (n, 1), 0)
    expert = divide(row, CHUNKS * capacity)
    row = row - expert * (CHUNKS * capacity)
    chunk = divide(row, capacity)
    slot = expert * capacity + row - chunk * capacity
    own = jnp.zeros((n, tok), F32)
    prob = jnp.zeros((n, tok), F32)
    for k in range(tops):
        hit = slot == position[k : k + 1, :]
        own = jnp.where(hit, 1.0, own)
        prob = jnp.where(hit, probs[k : k + 1, :], prob)
    total = jnp.zeros((n, part), F32)
    for c in range(CHUNKS):
        pick = jnp.where(chunk == c, own, 0.0).astype(BF)
        total = total + lax.dot_general(pick, wide[c * part : (c + 1) * part, :], NT, preferred_element_type=F32)
    if weigh:
        total = total * jnp.sum(prob, axis=1, keepdims=True)
    total = total.astype(BF)
    for d in range(out.shape[0]):
        out[d] = total


def build(weigh, rows_t, position, probs, capacity, rows, part, holders):
    width, tok = rows_t.shape
    tops = position.shape[0]
    span = rows // 4
    whole = lambda shape: pl.BlockSpec(shape, lambda i: (0,) * len(shape))
    return pl.pallas_call(
        functools.partial(build_kernel, weigh, part, capacity),
        grid=(rows // span,),
        out_shape=jax.ShapeDtypeStruct((holders, rows, part), BF),
        in_specs=[whole((width, tok)), whole((tops, tok)), whole((tops, tok))],
        out_specs=pl.BlockSpec((holders, span, part), lambda i: (0, i, 0)),
        scratch_shapes=[pltpu.VMEM((CHUNKS * part, tok), BF)],
        compiler_params=PARAMS,
        name="build_weighted" if weigh else "build_rows",
    )(rows_t, position, probs)


def body(tokens, cotangent, expert_ids, slots, probs, w_gate, w_up, w_down):
    experts = lax.axis_size("expert")
    holders = lax.axis_size("dp")
    tok_rows, width = tokens.shape
    top_count = expert_ids.shape[1]
    capacity = max(2, 3 * tok_rows * top_count // (4 * experts))
    part = -(-width // (CHUNKS * 128)) * 128
    devices = holders * experts
    block = CHUNKS * capacity
    send_rows = experts * block
    position = jnp.where(slots >= 0, expert_ids * capacity + slots, -1).T
    probs_t = probs.T

    row = jnp.arange(send_rows, dtype=jnp.int32)
    row_slot = (row // block) * capacity + row % capacity
    row_chunk = (row // capacity) % CHUNKS

    i = jnp.arange(GROUP * block, dtype=jnp.int32)
    source, chunk, slot = (i // capacity) % GROUP, i // (GROUP * capacity), i % capacity
    target = source * block + chunk * capacity + slot
    order = (target[:, None] == i[None, :]).astype(BF)
    order_t = (i[:, None] == target[None, :]).astype(BF)

    def exchange(blocks):
        blocks = blocks.reshape(devices, block, part)
        blocks = lax.all_to_all(blocks, ("dp", "expert"), split_axis=0, concat_axis=0, tiled=True)
        return blocks.reshape(devices * block, part)

    gate_w = w_gate[0].T
    up_w = w_up[0].T
    down_w = w_down[0].T
    place = (position, probs_t, capacity, send_rows, part, holders)
    token_half = build(False, tokens.T, *place)
    cot_half = build(True, cotangent.T, *place)
    token_recv = exchange(token_half)
    hits = (position.reshape(top_count * tok_rows, 1) == row_slot[None, :]).astype(BF)
    masks = (row_chunk[None, : send_rows // 4] == jnp.arange(CHUNKS)[:, None]).astype(BF)
    cot_half, token_recv = lax.optimization_barrier((cot_half, token_recv))
    cot_recv = exchange(cot_half)
    rows, hidden, glu, slope = gate_up(token_recv, order, gate_w, up_w)
    ret, weighted, gate_grad, up_grad = row_back(
        cot_recv, order, order_t, down_w, gate_w, up_w, hidden, glu, slope
    )
    back = exchange(ret)
    grad_down = lax.dot_general(weighted, hidden, TN, preferred_element_type=F32).astype(BF)
    grad_gate = lax.dot_general(rows, gate_grad, TN, preferred_element_type=F32).astype(BF)
    grad_up = lax.dot_general(rows, up_grad, TN, preferred_element_type=F32).astype(BF)
    input_grad, prob_grad = combine(back, hits, masks, probs_t, width)
    return (input_grad.T, prob_grad.T, grad_gate[None], grad_up[None], grad_down[None])


def solution(mesh):
    tokens = P(("expert", "dp"), None)
    weights = P("expert", None, "dp")
    return jax.shard_map(
        body,
        mesh=mesh,
        in_specs=(tokens,) * 5 + (weights,) * 3,
        out_specs=(tokens,) * 2 + (weights,) * 3,
        check_vma=False,
    )
```

```python
import functools

import jax
import jax.numpy as jnp
from jax import lax
from jax.experimental import pallas as pl
from jax.experimental.pallas import tpu as pltpu
from jax.sharding import PartitionSpec as P

ALPHA = 1.702
CHUNKS = 4
GROUP = 8
HALVES = 2
PIECES = 4
BF = jnp.bfloat16
F32 = jnp.float32
NT = (((1,), (1,)), ((), ()))
NN = (((1,), (0,)), ((), ()))
TN = (((0,), (0,)), ((), ()))
ANY = pl.BlockSpec(memory_space=pl.ANY)
VMEM = pl.BlockSpec(memory_space=pltpu.VMEM)
PARAMS = pltpu.CompilerParams(vmem_limit_bytes=60 * 1024 * 1024)


def sort_rows(recv, pick, out, p, pieces, part, width):
    size = pick.shape[0]
    lane_rows = size // CHUNKS
    groups = recv.shape[0] // GROUP

    def step(b, carry):
        blk = recv[pl.ds(b * GROUP, GROUP)].reshape(size, part)
        picked = lax.dot_general(pick, blk, NN, preferred_element_type=F32).astype(BF)
        at = pl.ds(pl.multiple_of(b * lane_rows, lane_rows), lane_rows)
        for c in range(CHUNKS):
            w = min(part, width - c * part)
            out[at, c * part : c * part + w] = picked[c * lane_rows : (c + 1) * lane_rows, :w]
        return carry

    lax.fori_loop(p * groups // pieces, (p + 1) * groups // pieces, step, 0, unroll=2)


def expert_kernel(
    part, recv_hbm, order, order_t, wg_hbm, wu_hbm, wd_hbm,
    ret_hbm, rows_hbm, weighted_hbm, hidden_hbm, gate_hbm, up_hbm,
    recv_t, recv_c, wg, wu, wd, rows, weighted, hidden, glu, slope, gate_grad, up_grad, wide, ret,
    in_sems, t_sems, c_sems, out_sems,
):
    units, width = wg.shape
    total = rows.shape[0]
    m = total // HALVES
    last = width - (CHUNKS - 1) * part
    mark = -(-last // 128) * 128
    size = order.shape[0]
    lane_rows = size // CHUNKS
    block = recv_t.shape[1]
    sources = recv_t.shape[0]
    span = sources // PIECES

    def pieces(dst, first, sems):
        return [
            pltpu.make_async_copy(
                recv_hbm.at[pl.ds(p * span, span), pl.ds(first, block)], dst.at[pl.ds(p * span, span)], sems.at[p]
            )
            for p in range(PIECES)
        ]

    def load(src, dst, i):
        return pltpu.make_async_copy(src, dst, in_sems.at[i])

    stores = []

    def store(src, dst):
        stores.append(pltpu.make_async_copy(src, dst, out_sems.at[len(stores)]))
        stores[-1].start()

    t_loads = pieces(recv_t, 0, t_sems)
    c_loads = pieces(recv_c, block, c_sems)
    g_load, u_load, d_load = load(wg_hbm, wg, 0), load(wu_hbm, wu, 1), load(wd_hbm, wd, 2)
    for copy in (*t_loads, g_load, u_load, *c_loads, d_load):
        copy.start()
    pick = order[...]
    pick_t = order_t[...]
    for p in range(PIECES):
        t_loads[p].wait()
        sort_rows(recv_t, pick, rows, p, PIECES, part, width)
    store(rows, rows_hbm)
    for i in range(HALVES):
        at = pl.ds(i * m, m)
        if i == 0:
            g_load.wait()
        g = lax.dot_general(rows[at, :], wg[...], NT, preferred_element_type=F32)
        if i == 0:
            u_load.wait()
        u = lax.dot_general(rows[at, :], wu[...], NT, preferred_element_type=F32) + 1.0
        s = jax.nn.sigmoid(ALPHA * g)
        gl = g * s
        hidden[at, :] = (u * gl).astype(BF)
        glu[at, :] = gl
        slope[at, :] = u * (s + ALPHA * g * s * (1.0 - s))
    store(hidden, hidden_hbm)
    for p in range(PIECES):
        c_loads[p].wait()
        sort_rows(recv_c, pick, weighted, p, PIECES, part, width)
    store(weighted, weighted_hbm)
    for i in range(HALVES):
        at = pl.ds(i * m, m)
        if i == 0:
            d_load.wait()
        hg = lax.dot_general(weighted[at, :], wd[...], NT, preferred_element_type=F32)
        sg = jnp.sum(hg * hidden[at, :].astype(F32), axis=1, keepdims=True)
        ug = (hg * glu[at, :]).astype(BF)
        gg = (hg * slope[at, :]).astype(BF)
        gate_grad[at, :] = gg
        up_grad[at, :] = ug
        store(gate_grad.at[at], gate_hbm.at[at])
        store(up_grad.at[at], up_hbm.at[at])
        low = sg - sg.astype(BF).astype(F32)
        lane = lax.broadcasted_iota(jnp.int32, (m, part - mark), 1)
        tail = jnp.where(lane == 0, sg, jnp.where(lane == 1, low, 0.0)).astype(BF)
        if last < mark:
            wide[CHUNKS - 1, :, mark - 128 : mark] = jnp.zeros((m, 128), BF)
        wide[CHUNKS - 1, :, mark:] = tail
        for c in range(CHUNKS):
            w = min(part, width - c * part)
            x = lax.dot_general(gg, wg[:, c * part : c * part + w], NN, preferred_element_type=F32)
            x = x + lax.dot_general(ug, wu[:, c * part : c * part + w], NN, preferred_element_type=F32)
            wide[c, :, :w] = x.astype(BF)
        first = i * (ret.shape[0] // HALVES)

        def put(b, carry):
            src = pl.ds(pl.multiple_of(b * lane_rows, lane_rows), lane_rows)
            blk = jnp.concatenate([wide[c, src, :] for c in range(CHUNKS)], axis=0)
            out = lax.dot_general(pick_t, blk, NN, preferred_element_type=F32)
            ret[pl.ds(pl.multiple_of(first + b * size, size), size), :] = out.astype(BF)
            return carry

        lax.fori_loop(0, m // lane_rows, put, 0, unroll=2)
        half = pl.ds(first, ret.shape[0] // HALVES)
        store(ret.at[half], ret_hbm.at[half])
    for copy in stores:
        copy.wait()


def expert(recv, order, order_t, wg, wu, wd):
    units, width = wg.shape
    sources, both, part = recv.shape
    block = both // 2
    total = sources * block // CHUNKS
    like = jax.ShapeDtypeStruct
    scratch = lambda shape, dtype=BF: pltpu.VMEM(shape, dtype)
    return pl.pallas_call(
        functools.partial(expert_kernel, part),
        out_shape=(
            like((sources * block, part), BF),
            like((total, width), BF),
            like((total, width), BF),
            like((total, units), BF),
            like((total, units), BF),
            like((total, units), BF),
        ),
        in_specs=[ANY, VMEM, VMEM, ANY, ANY, ANY],
        out_specs=(ANY,) * 6,
        scratch_shapes=[
            scratch((sources, block, part)),
            scratch((sources, block, part)),
            scratch((units, width)),
            scratch((units, width)),
            scratch((units, width)),
            scratch((total, width)),
            scratch((total, width)),
            scratch((total, units)),
            scratch((total, units), F32),
            scratch((total, units), F32),
            scratch((total, units)),
            scratch((total, units)),
            scratch((CHUNKS, total // HALVES, part)),
            scratch((sources * block, part)),
            pltpu.SemaphoreType.DMA((3,)),
            pltpu.SemaphoreType.DMA((PIECES,)),
            pltpu.SemaphoreType.DMA((PIECES,)),
            pltpu.SemaphoreType.DMA((3 + 3 * HALVES,)),
        ],
        compiler_params=PARAMS,
        name="expert",
    )(recv, order, order_t, wg, wu, wd)


def combine_kernel(part, width, back, hits, masks, probs, input_grad, prob_grad, acc, pacc):
    step = pl.program_id(0)
    tops, tok = probs.shape
    last = width - (CHUNKS - 1) * part
    mark = -(-last // 128) * 128

    @pl.when(step == 0)
    def _():
        acc[...] = jnp.zeros_like(acc)
        pacc[...] = jnp.zeros_like(pacc)

    hit = hits[...]
    own = hit[:tok]
    for k in range(1, tops):
        own = own + hit[k * tok : (k + 1) * tok]
    mask = masks[...]
    spread = jnp.concatenate([own * mask[c : c + 1] for c in range(CHUNKS)], axis=0)
    blk = back[...]
    acc[...] += lax.dot_general(spread, blk, NN, preferred_element_type=F32)
    pacc[...] += lax.dot_general(hit * mask[CHUNKS - 1 : CHUNKS], blk[:, mark : mark + 128], NN, preferred_element_type=F32)

    @pl.when(step == pl.num_programs(0) - 1)
    def _():
        for c in range(CHUNKS):
            w = min(part, width - c * part)
            input_grad[c * part : c * part + w, :] = acc[c * tok : (c + 1) * tok, :].T[:w].astype(BF)
        for k in range(tops):
            col = pacc[k * tok : (k + 1) * tok, :].T
            prob_grad[k : k + 1, :] = (col[0:1] + col[1:2]) / probs[k : k + 1, :]

def combine(back, hits, masks, probs_t, width):
    rows, part = back.shape
    tops, tok = probs_t.shape
    span = masks.shape[1]
    turns = hits.shape[1] // span
    like = jax.ShapeDtypeStruct
    return pl.pallas_call(
        functools.partial(combine_kernel, part, width),
        grid=(rows // span,),
        out_shape=(like((width, tok), BF), like((tops, tok), F32)),
        in_specs=[
            pl.BlockSpec((span, part), lambda i: (i, 0)),
            pl.BlockSpec((tops * tok, span), lambda i: (0, i % turns)),
            pl.BlockSpec((CHUNKS, span), lambda i: (0, 0)),
            pl.BlockSpec((tops, tok), lambda i: (0, 0)),
        ],
        out_specs=(pl.BlockSpec((width, tok), lambda i: (0, 0)), pl.BlockSpec((tops, tok), lambda i: (0, 0))),
        scratch_shapes=[pltpu.VMEM((CHUNKS * tok, part), F32), pltpu.VMEM((tops * tok, 128), F32)],
        compiler_params=pltpu.CompilerParams(vmem_limit_bytes=24 * 1024 * 1024),
        name="combine",
    )(back, hits, masks, probs_t)

def divide(x, by):
    return jnp.floor((x.astype(F32) + 0.5) * (1.0 / by)).astype(jnp.int32)


def build_kernel(part, capacity, tokens_t, cotangent_t, position, probs, out, wide):
    width, tok = tokens_t.shape
    tops = position.shape[0]

    @pl.when(pl.program_id(0) == 0)
    def _():
        for j, src in enumerate((tokens_t, cotangent_t)):
            for c in range(CHUNKS):
                w = min(part, width - c * part)
                wide[j, c * tok : (c + 1) * tok, :w] = src[c * part : c * part + w, :].T
                if w < part:
                    wide[j, c * tok : (c + 1) * tok, w:] = jnp.zeros((tok, part - w), BF)

    experts, both = out.shape[1:3]
    block = both // 2
    n = experts * block
    row = pl.program_id(0) * n + lax.broadcasted_iota(jnp.int32, (n, 1), 0)
    expert = divide(row, block)
    row = row - expert * block
    chunk = divide(row, capacity)
    slot = expert * capacity + row - chunk * capacity
    own = jnp.zeros((n, tok), F32)
    prob = jnp.zeros((n, tok), F32)
    for k in range(tops):
        hit = slot == position[k : k + 1, :]
        own = jnp.where(hit, 1.0, own)
        prob = jnp.where(hit, probs[k : k + 1, :], prob)
    pick = jnp.concatenate([jnp.where(chunk == c, own, 0.0).astype(BF) for c in range(CHUNKS)], axis=1)
    sent = lax.dot_general(pick, wide[0], NN, preferred_element_type=F32).astype(BF)
    cot = lax.dot_general(pick, wide[1], NN, preferred_element_type=F32)
    cot = (cot * jnp.sum(prob, axis=1, keepdims=True)).astype(BF)
    for d in range(out.shape[0]):
        out[d, :, :block, :] = sent.reshape(experts, block, part)
        out[d, :, block:, :] = cot.reshape(experts, block, part)


def build(tokens_t, cotangent_t, position, probs, capacity, experts, part, holders):
    width, tok = tokens_t.shape
    tops = position.shape[0]
    both = 2 * CHUNKS * capacity
    steps = 4
    whole = lambda shape: pl.BlockSpec(shape, lambda i: (0,) * len(shape))
    return pl.pallas_call(
        functools.partial(build_kernel, part, capacity),
        grid=(steps,),
        out_shape=jax.ShapeDtypeStruct((holders, experts, both, part), BF),
        in_specs=[whole((width, tok)), whole((width, tok)), whole((tops, tok)), whole((tops, tok))],
        out_specs=pl.BlockSpec((holders, experts // steps, both, part), lambda i: (0, i, 0, 0)),
        scratch_shapes=[pltpu.VMEM((2, CHUNKS * tok, part), BF)],
        compiler_params=PARAMS,
        name="build",
    )(tokens_t, cotangent_t, position, probs)


def body(tokens, cotangent, expert_ids, slots, probs, w_gate, w_up, w_down):
    experts = lax.axis_size("expert")
    holders = lax.axis_size("dp")
    tok_rows, width = tokens.shape
    top_count = expert_ids.shape[1]
    capacity = max(2, 3 * tok_rows * top_count // (4 * experts))
    part = -(-width // (CHUNKS * 128)) * 128
    devices = holders * experts
    block = CHUNKS * capacity
    send_rows = experts * block
    position = jnp.where(slots >= 0, expert_ids * capacity + slots, -1).T
    probs_t = probs.T

    row = jnp.arange(send_rows, dtype=jnp.int32)
    row_slot = (row // block) * capacity + row % capacity
    row_chunk = (row // capacity) % CHUNKS

    i = jnp.arange(GROUP * block, dtype=jnp.int32)
    source, chunk, slot = (i // capacity) % GROUP, i // (GROUP * capacity), i % capacity
    target = source * block + chunk * capacity + slot
    order = (target[:, None] == i[None, :]).astype(BF)
    order_t = (i[:, None] == target[None, :]).astype(BF)

    def exchange(blocks):
        return lax.all_to_all(blocks, ("dp", "expert"), split_axis=0, concat_axis=0, tiled=True)

    gate_w = w_gate[0].T
    up_w = w_up[0].T
    down_w = w_down[0].T
    sent = build(tokens.T, cotangent.T, position, probs_t, capacity, experts, part, holders)
    recv = exchange(sent.reshape(devices, 2 * block, part))
    hits = (position.reshape(top_count * tok_rows, 1) == row_slot[None, :]).astype(BF)
    masks = (row_chunk[None, : send_rows // 4] == jnp.arange(CHUNKS)[:, None]).astype(BF)
    ret, rows, weighted, hidden, gate_grad, up_grad = expert(recv, order, order_t, gate_w, up_w, down_w)
    back = exchange(ret.reshape(devices, block, part)).reshape(devices * block, part)
    with jax.named_scope("weight_grads"):
        grad_down = lax.dot_general(weighted, hidden, TN, preferred_element_type=F32).astype(BF)
        grad_gate = lax.dot_general(rows, gate_grad, TN, preferred_element_type=F32).astype(BF)
        grad_up = lax.dot_general(rows, up_grad, TN, preferred_element_type=F32).astype(BF)
    with jax.named_scope("combine"):
        input_grad, prob_grad = combine(back, hits, masks, probs_t, width)
    return (input_grad.T, prob_grad.T, grad_gate[None], grad_up[None], grad_down[None])


def solution(mesh):
    tokens = P(("expert", "dp"), None)
    weights = P("expert", None, "dp")
    return jax.shard_map(
        body,
        mesh=mesh,
        in_specs=(tokens,) * 5 + (weights,) * 3,
        out_specs=(tokens,) * 2 + (weights,) * 3,
        check_vma=False,
    )
```

```python
import functools

import jax
import jax.numpy as jnp
import numpy as np
from jax import lax
from jax.experimental import pallas as pl
from jax.experimental.pallas import tpu as pltpu
from jax.sharding import PartitionSpec as P

ALPHA = 1.702
CHUNKS = 4
GROUP = 8
HALVES = 2
PIECES = 4
BF = jnp.bfloat16
F32 = jnp.float32
NT = (((1,), (1,)), ((), ()))
NN = (((1,), (0,)), ((), ()))
TN = (((0,), (0,)), ((), ()))
ANY = pl.BlockSpec(memory_space=pl.ANY)
VMEM = pl.BlockSpec(memory_space=pltpu.VMEM)
PARAMS = pltpu.CompilerParams(vmem_limit_bytes=60 * 1024 * 1024)


def sort_rows(recv, pick, out, p, pieces, part, width):
    size = pick.shape[0]
    lane_rows = size // CHUNKS
    groups = recv.shape[0] // GROUP

    def step(b, carry):
        blk = recv[pl.ds(b * GROUP, GROUP)].reshape(size, part)
        picked = lax.dot_general(pick, blk, NN, preferred_element_type=F32).astype(BF)
        at = pl.ds(pl.multiple_of(b * lane_rows, lane_rows), lane_rows)
        for c in range(CHUNKS):
            w = min(part, width - c * part)
            out[at, c * part : c * part + w] = picked[c * lane_rows : (c + 1) * lane_rows, :w]
        return carry

    lax.fori_loop(p * groups // pieces, (p + 1) * groups // pieces, step, 0, unroll=2)


def expert_kernel(
    part, recv_hbm, order, order_t, wg_hbm, wu_hbm, wd_hbm,
    ret_hbm, rows_hbm, weighted_hbm, hidden_hbm, gate_hbm, up_hbm,
    recv_t, recv_c, wg, wu, wd, rows, weighted, hidden, glu, slope, gate_grad, up_grad, wide, ret,
    in_sems, t_sems, c_sems, out_sems,
):
    units, width = wg.shape
    total = rows.shape[0]
    m = total // HALVES
    last = width - (CHUNKS - 1) * part
    mark = -(-last // 128) * 128
    size = order.shape[0]
    lane_rows = size // CHUNKS
    block = recv_t.shape[1]
    sources = recv_t.shape[0]
    span = sources // PIECES

    def pieces(dst, first, sems):
        return [
            pltpu.make_async_copy(
                recv_hbm.at[pl.ds(p * span, span), pl.ds(first, block)], dst.at[pl.ds(p * span, span)], sems.at[p]
            )
            for p in range(PIECES)
        ]

    def load(src, dst, i):
        return pltpu.make_async_copy(src, dst, in_sems.at[i])

    stores = []

    def store(src, dst):
        stores.append(pltpu.make_async_copy(src, dst, out_sems.at[len(stores)]))
        stores[-1].start()

    t_loads = pieces(recv_t, 0, t_sems)
    c_loads = pieces(recv_c, block, c_sems)
    g_load, u_load, d_load = load(wg_hbm, wg, 0), load(wu_hbm, wu, 1), load(wd_hbm, wd, 2)
    for copy in (*t_loads, g_load, u_load, *c_loads, d_load):
        copy.start()
    pick = order[...]
    pick_t = order_t[...]
    for p in range(PIECES):
        t_loads[p].wait()
        sort_rows(recv_t, pick, rows, p, PIECES, part, width)
    store(rows, rows_hbm)
    for i in range(HALVES):
        at = pl.ds(i * m, m)
        if i == 0:
            g_load.wait()
        g = lax.dot_general(rows[at, :], wg[...], NT, preferred_element_type=F32)
        if i == 0:
            u_load.wait()
        u = lax.dot_general(rows[at, :], wu[...], NT, preferred_element_type=F32) + 1.0
        s = jax.nn.sigmoid(ALPHA * g)
        gl = g * s
        hidden[at, :] = (u * gl).astype(BF)
        glu[at, :] = gl
        slope[at, :] = u * (s + ALPHA * g * s * (1.0 - s))
    store(hidden, hidden_hbm)
    for p in range(PIECES):
        c_loads[p].wait()
        sort_rows(recv_c, pick, weighted, p, PIECES, part, width)
    store(weighted, weighted_hbm)
    for i in range(HALVES):
        at = pl.ds(i * m, m)
        if i == 0:
            d_load.wait()
        hg = lax.dot_general(weighted[at, :], wd[...], NT, preferred_element_type=F32)
        sg = jnp.sum(hg * hidden[at, :].astype(F32), axis=1, keepdims=True)
        ug = (hg * glu[at, :]).astype(BF)
        gg = (hg * slope[at, :]).astype(BF)
        gate_grad[at, :] = gg
        up_grad[at, :] = ug
        store(gate_grad.at[at], gate_hbm.at[at])
        store(up_grad.at[at], up_hbm.at[at])
        low = sg - sg.astype(BF).astype(F32)
        lane = lax.broadcasted_iota(jnp.int32, (m, part - mark), 1)
        tail = jnp.where(lane == 0, sg, jnp.where(lane == 1, low, 0.0)).astype(BF)
        if last < mark:
            wide[CHUNKS - 1, :, mark - 128 : mark] = jnp.zeros((m, 128), BF)
        wide[CHUNKS - 1, :, mark:] = tail
        for c in range(CHUNKS):
            w = min(part, width - c * part)
            x = lax.dot_general(gg, wg[:, c * part : c * part + w], NN, preferred_element_type=F32)
            x = x + lax.dot_general(ug, wu[:, c * part : c * part + w], NN, preferred_element_type=F32)
            wide[c, :, :w] = x.astype(BF)
        first = i * (ret.shape[0] // HALVES)

        def put(b, carry):
            src = pl.ds(pl.multiple_of(b * lane_rows, lane_rows), lane_rows)
            blk = jnp.concatenate([wide[c, src, :] for c in range(CHUNKS)], axis=0)
            out = lax.dot_general(pick_t, blk, NN, preferred_element_type=F32)
            ret[pl.ds(pl.multiple_of(first + b * size, size), size), :] = out.astype(BF)
            return carry

        lax.fori_loop(0, m // lane_rows, put, 0, unroll=2)
        half = pl.ds(first, ret.shape[0] // HALVES)
        store(ret.at[half], ret_hbm.at[half])
    for copy in stores:
        copy.wait()


def expert(recv, order, order_t, wg, wu, wd):
    units, width = wg.shape
    sources, both, part = recv.shape
    block = both // 2
    total = sources * block // CHUNKS
    like = jax.ShapeDtypeStruct
    scratch = lambda shape, dtype=BF: pltpu.VMEM(shape, dtype)
    return pl.pallas_call(
        functools.partial(expert_kernel, part),
        out_shape=(
            like((sources * block, part), BF),
            like((total, width), BF),
            like((total, width), BF),
            like((total, units), BF),
            like((total, units), BF),
            like((total, units), BF),
        ),
        in_specs=[ANY, VMEM, VMEM, ANY, ANY, ANY],
        out_specs=(ANY,) * 6,
        scratch_shapes=[
            scratch((sources, block, part)),
            scratch((sources, block, part)),
            scratch((units, width)),
            scratch((units, width)),
            scratch((units, width)),
            scratch((total, width)),
            scratch((total, width)),
            scratch((total, units)),
            scratch((total, units), F32),
            scratch((total, units), F32),
            scratch((total, units)),
            scratch((total, units)),
            scratch((CHUNKS, total // HALVES, part)),
            scratch((sources * block, part)),
            pltpu.SemaphoreType.DMA((3,)),
            pltpu.SemaphoreType.DMA((PIECES,)),
            pltpu.SemaphoreType.DMA((PIECES,)),
            pltpu.SemaphoreType.DMA((3 + 3 * HALVES,)),
        ],
        compiler_params=PARAMS,
        name="expert",
    )(recv, order, order_t, wg, wu, wd)


def combine_kernel(part, width, back, hits, masks, probs, input_grad, prob_grad, acc, pacc):
    step = pl.program_id(0)
    tops, tok = probs.shape
    last = width - (CHUNKS - 1) * part
    mark = -(-last // 128) * 128

    @pl.when(step == 0)
    def _():
        acc[...] = jnp.zeros_like(acc)
        pacc[...] = jnp.zeros_like(pacc)

    hit = hits[...]
    own = hit[:tok]
    for k in range(1, tops):
        own = own + hit[k * tok : (k + 1) * tok]
    mask = masks[...]
    spread = jnp.concatenate([own * mask[c : c + 1] for c in range(CHUNKS)], axis=0)
    blk = back[...]
    acc[...] += lax.dot_general(spread, blk, NN, preferred_element_type=F32)
    pacc[...] += lax.dot_general(hit * mask[CHUNKS - 1 : CHUNKS], blk[:, mark : mark + 128], NN, preferred_element_type=F32)

    @pl.when(step == pl.num_programs(0) - 1)
    def _():
        for c in range(CHUNKS):
            w = min(part, width - c * part)
            input_grad[c * part : c * part + w, :] = acc[c * tok : (c + 1) * tok, :].T[:w].astype(BF)
        for k in range(tops):
            col = pacc[k * tok : (k + 1) * tok, :].T
            prob_grad[k : k + 1, :] = (col[0:1] + col[1:2]) / probs[k : k + 1, :]

def combine(back, hits, masks, probs_t, width):
    rows, part = back.shape
    tops, tok = probs_t.shape
    span = masks.shape[1]
    turns = hits.shape[1] // span
    like = jax.ShapeDtypeStruct
    return pl.pallas_call(
        functools.partial(combine_kernel, part, width),
        grid=(rows // span,),
        out_shape=(like((width, tok), BF), like((tops, tok), F32)),
        in_specs=[
            pl.BlockSpec((span, part), lambda i: (i, 0)),
            pl.BlockSpec((tops * tok, span), lambda i: (0, i % turns)),
            pl.BlockSpec((CHUNKS, span), lambda i: (0, 0)),
            pl.BlockSpec((tops, tok), lambda i: (0, 0)),
        ],
        out_specs=(pl.BlockSpec((width, tok), lambda i: (0, 0)), pl.BlockSpec((tops, tok), lambda i: (0, 0))),
        scratch_shapes=[pltpu.VMEM((CHUNKS * tok, part), F32), pltpu.VMEM((tops * tok, 128), F32)],
        compiler_params=pltpu.CompilerParams(vmem_limit_bytes=24 * 1024 * 1024),
        name="combine",
    )(back, hits, masks, probs_t)

def divide(x, by):
    return jnp.floor((x.astype(F32) + 0.5) * (1.0 / by)).astype(jnp.int32)


def build_kernel(part, capacity, tokens_t, cotangent_t, position, probs, out, wide):
    width, tok = tokens_t.shape
    tops = position.shape[0]

    @pl.when(pl.program_id(0) == 0)
    def _():
        for j, src in enumerate((tokens_t, cotangent_t)):
            for c in range(CHUNKS):
                w = min(part, width - c * part)
                wide[j, c * tok : (c + 1) * tok, :w] = src[c * part : c * part + w, :].T
                if w < part:
                    wide[j, c * tok : (c + 1) * tok, w:] = jnp.zeros((tok, part - w), BF)

    experts, both = out.shape[1:3]
    block = both // 2
    n = experts * block
    row = pl.program_id(0) * n + lax.broadcasted_iota(jnp.int32, (n, 1), 0)
    expert = divide(row, block)
    row = row - expert * block
    chunk = divide(row, capacity)
    slot = expert * capacity + row - chunk * capacity
    own = jnp.zeros((n, tok), F32)
    prob = jnp.zeros((n, tok), F32)
    for k in range(tops):
        hit = slot == position[k : k + 1, :]
        own = jnp.where(hit, 1.0, own)
        prob = jnp.where(hit, probs[k : k + 1, :], prob)
    pick = jnp.concatenate([jnp.where(chunk == c, own, 0.0).astype(BF) for c in range(CHUNKS)], axis=1)
    sent = lax.dot_general(pick, wide[0], NN, preferred_element_type=F32).astype(BF)
    cot = lax.dot_general(pick, wide[1], NN, preferred_element_type=F32)
    cot = (cot * jnp.sum(prob, axis=1, keepdims=True)).astype(BF)
    for d in range(out.shape[0]):
        out[d, :, :block, :] = sent.reshape(experts, block, part)
        out[d, :, block:, :] = cot.reshape(experts, block, part)


def build(tokens_t, cotangent_t, position, probs, capacity, experts, part, holders):
    width, tok = tokens_t.shape
    tops = position.shape[0]
    both = 2 * CHUNKS * capacity
    steps = 4
    whole = lambda shape: pl.BlockSpec(shape, lambda i: (0,) * len(shape))
    return pl.pallas_call(
        functools.partial(build_kernel, part, capacity),
        grid=(steps,),
        out_shape=jax.ShapeDtypeStruct((holders, experts, both, part), BF),
        in_specs=[whole((width, tok)), whole((width, tok)), whole((tops, tok)), whole((tops, tok))],
        out_specs=pl.BlockSpec((holders, experts // steps, both, part), lambda i: (0, i, 0, 0)),
        scratch_shapes=[pltpu.VMEM((2, CHUNKS * tok, part), BF)],
        compiler_params=PARAMS,
        name="build",
    )(tokens_t, cotangent_t, position, probs)


def body(tokens, cotangent, expert_ids, slots, probs, w_gate, w_up, w_down):
    experts = lax.axis_size("expert")
    holders = lax.axis_size("dp")
    tok_rows, width = tokens.shape
    top_count = expert_ids.shape[1]
    capacity = max(2, 3 * tok_rows * top_count // (4 * experts))
    part = -(-width // (CHUNKS * 128)) * 128
    devices = holders * experts
    block = CHUNKS * capacity
    send_rows = experts * block
    position = jnp.where(slots >= 0, expert_ids * capacity + slots, -1).T
    probs_t = probs.T

    row = jnp.arange(send_rows, dtype=jnp.int32)
    row_slot = (row // block) * capacity + row % capacity
    row_chunk = (row // capacity) % CHUNKS

    i = np.arange(GROUP * block)
    source, chunk, slot = (i // capacity) % GROUP, i // (GROUP * capacity), i % capacity
    target = source * block + chunk * capacity + slot
    order = jnp.asarray(target[:, None] == i[None, :], BF)
    order_t = jnp.asarray(i[:, None] == target[None, :], BF)

    def exchange(blocks):
        return lax.all_to_all(blocks, ("dp", "expert"), split_axis=0, concat_axis=0, tiled=True)

    gate_w = w_gate[0].T
    up_w = w_up[0].T
    down_w = w_down[0].T
    sent = build(tokens.T, cotangent.T, position, probs_t, capacity, experts, part, holders)
    recv = exchange(sent.reshape(devices, 2 * block, part))
    hits = (position.reshape(top_count * tok_rows, 1) == row_slot[None, :]).astype(BF)
    masks = (row_chunk[None, : send_rows // 4] == jnp.arange(CHUNKS)[:, None]).astype(BF)
    ret, rows, weighted, hidden, gate_grad, up_grad = expert(recv, order, order_t, gate_w, up_w, down_w)
    back = exchange(ret.reshape(devices, block, part)).reshape(devices * block, part)
    with jax.named_scope("weight_grads"):
        grad_down = lax.dot_general(weighted, hidden, TN, preferred_element_type=F32).astype(BF)
        grad_gate = lax.dot_general(rows, gate_grad, TN, preferred_element_type=F32).astype(BF)
        grad_up = lax.dot_general(rows, up_grad, TN, preferred_element_type=F32).astype(BF)
    with jax.named_scope("combine"):
        input_grad, prob_grad = combine(back, hits, masks, probs_t, width)
    return (input_grad.T, prob_grad.T, grad_gate[None], grad_up[None], grad_down[None])


def solution(mesh):
    tokens = P(("expert", "dp"), None)
    weights = P("expert", None, "dp")
    return jax.shard_map(
        body,
        mesh=mesh,
        in_specs=(tokens,) * 5 + (weights,) * 3,
        out_specs=(tokens,) * 2 + (weights,) * 3,
        check_vma=False,
    )
```

```python
import functools

import jax
import jax.numpy as jnp
import numpy as np
from jax import lax
from jax.experimental import pallas as pl
from jax.experimental.pallas import tpu as pltpu
from jax.sharding import PartitionSpec as P

ALPHA = 1.702
CHUNKS = 4
GROUP = 8
HALVES = 2
PARTS = 2
UNROLL = 8
STEPS = 4
TURNS = 1
BF = jnp.bfloat16
F32 = jnp.float32
NT = (((1,), (1,)), ((), ()))
NN = (((1,), (0,)), ((), ()))
TN = (((0,), (0,)), ((), ()))
ANY = pl.BlockSpec(memory_space=pl.ANY)
VMEM = pl.BlockSpec(memory_space=pltpu.VMEM)
PARAMS = pltpu.CompilerParams(vmem_limit_bytes=60 * 1024 * 1024)


def sort_rows(recv, pick, out, i, part, width):
    size = pick.shape[0]
    lane_rows = size // CHUNKS
    groups = recv.shape[0] // GROUP

    def step(b, carry):
        blk = recv[pl.ds(b * GROUP, GROUP)].reshape(size, part)
        picked = lax.dot_general(pick, blk, NN, preferred_element_type=F32).astype(BF)
        at = pl.ds(pl.multiple_of(b * lane_rows, lane_rows), lane_rows)
        for c in range(CHUNKS):
            w = min(part, width - c * part)
            out[at, c * part : c * part + w] = picked[c * lane_rows : (c + 1) * lane_rows, :w]
        return carry

    lax.fori_loop(i * groups // HALVES, (i + 1) * groups // HALVES, step, 0, unroll=UNROLL)


def expert_kernel(
    part, recv_hbm, order, order_t, wg_hbm, wu_hbm, wd_hbm,
    ret_hbm, rows_hbm, weighted_hbm, hidden_hbm, gate_hbm, up_hbm,
    recv_t, recv_c, wg, wu, wd, rows, weighted, hidden, glu, slope, gate_grad, up_grad, wide, ret,
    in_sems, t_sems, c_sems, out_sems,
):
    units, width = wg.shape
    total = rows.shape[0]
    m = total // HALVES
    last = width - (CHUNKS - 1) * part
    mark = -(-last // 128) * 128
    size = order.shape[0]
    lane_rows = size // CHUNKS
    block = recv_t.shape[1]
    sources = recv_t.shape[0]
    span = sources // HALVES

    def pieces(dst, first, sems):
        return [
            pltpu.make_async_copy(
                recv_hbm.at[pl.ds(p * span, span), pl.ds(first, block)], dst.at[pl.ds(p * span, span)], sems.at[p]
            )
            for p in range(HALVES)
        ]

    def load(src, dst, i):
        return pltpu.make_async_copy(src, dst, in_sems.at[i])

    stores = []

    def store(src, dst):
        stores.append(pltpu.make_async_copy(src, dst, out_sems.at[len(stores)]))
        stores[-1].start()

    t_loads = pieces(recv_t, 0, t_sems)
    c_loads = pieces(recv_c, block, c_sems)
    g_load, u_load, d_load = load(wg_hbm, wg, 0), load(wu_hbm, wu, 1), load(wd_hbm, wd, 2)
    for copy in (t_loads[0], g_load, u_load, *t_loads[1:], d_load, *c_loads):
        copy.start()
    pick = order[...]
    pick_t = order_t[...]
    for i in range(HALVES):
        at = pl.ds(i * m, m)
        t_loads[i].wait()
        sort_rows(recv_t, pick, rows, i, part, width)
        store(rows.at[at], rows_hbm.at[at])
        if i == 0:
            g_load.wait()
        g = lax.dot_general(rows[at, :], wg[...], NT, preferred_element_type=F32)
        if i == 0:
            u_load.wait()
        u = lax.dot_general(rows[at, :], wu[...], NT, preferred_element_type=F32) + 1.0
        s = jax.nn.sigmoid(ALPHA * g)
        gl = g * s
        hidden[at, :] = (u * gl).astype(BF)
        glu[at, :] = gl
        slope[at, :] = u * (s + ALPHA * g * s * (1.0 - s))
        store(hidden.at[at], hidden_hbm.at[at])
    for i in range(HALVES):
        at = pl.ds(i * m, m)
        c_loads[i].wait()
        sort_rows(recv_c, pick, weighted, i, part, width)
        store(weighted.at[at], weighted_hbm.at[at])
        if i == 0:
            d_load.wait()
        hg = lax.dot_general(weighted[at, :], wd[...], NT, preferred_element_type=F32)
        sg = jnp.sum(hg * hidden[at, :].astype(F32), axis=1, keepdims=True)
        ug = (hg * glu[at, :]).astype(BF)
        gg = (hg * slope[at, :]).astype(BF)
        gate_grad[at, :] = gg
        up_grad[at, :] = ug
        store(gate_grad.at[at], gate_hbm.at[at])
        store(up_grad.at[at], up_hbm.at[at])
        low = sg - sg.astype(BF).astype(F32)
        lane = lax.broadcasted_iota(jnp.int32, (m, part - mark), 1)
        tail = jnp.where(lane == 0, sg, jnp.where(lane == 1, low, 0.0)).astype(BF)
        if last < mark:
            wide[CHUNKS - 1, :, mark - 128 : mark] = jnp.zeros((m, 128), BF)
        wide[CHUNKS - 1, :, mark:] = tail
        for c in range(CHUNKS):
            w = min(part, width - c * part)
            x = lax.dot_general(gg, wg[:, c * part : c * part + w], NN, preferred_element_type=F32)
            x = x + lax.dot_general(ug, wu[:, c * part : c * part + w], NN, preferred_element_type=F32)
            wide[c, :, :w] = x.astype(BF)
        first = i * (ret.shape[0] // HALVES)

        def put(b, carry):
            src = pl.ds(pl.multiple_of(b * lane_rows, lane_rows), lane_rows)
            blk = jnp.concatenate([wide[c, src, :] for c in range(CHUNKS)], axis=0)
            out = lax.dot_general(pick_t, blk, NN, preferred_element_type=F32)
            ret[pl.ds(pl.multiple_of(first + b * size, size), size), :] = out.astype(BF)
            return carry

        turns = m // lane_rows // PARTS
        for q in range(PARTS):
            lax.fori_loop(q * turns, (q + 1) * turns, put, 0, unroll=turns)
            done = pl.ds(first + q * turns * size, turns * size)
            store(ret.at[done], ret_hbm.at[done])
    for copy in stores:
        copy.wait()


def expert(recv, order, order_t, wg, wu, wd):
    units, width = wg.shape
    sources, both, part = recv.shape
    block = both // 2
    total = sources * block // CHUNKS
    like = jax.ShapeDtypeStruct
    scratch = lambda shape, dtype=BF: pltpu.VMEM(shape, dtype)
    return pl.pallas_call(
        functools.partial(expert_kernel, part),
        out_shape=(
            like((sources * block, part), BF),
            like((total, width), BF),
            like((total, width), BF),
            like((total, units), BF),
            like((total, units), BF),
            like((total, units), BF),
        ),
        in_specs=[ANY, VMEM, VMEM, ANY, ANY, ANY],
        out_specs=(ANY,) * 6,
        scratch_shapes=[
            scratch((sources, block, part)),
            scratch((sources, block, part)),
            scratch((units, width)),
            scratch((units, width)),
            scratch((units, width)),
            scratch((total, width)),
            scratch((total, width)),
            scratch((total, units)),
            scratch((total, units), F32),
            scratch((total, units), F32),
            scratch((total, units)),
            scratch((total, units)),
            scratch((CHUNKS, total // HALVES, part)),
            scratch((sources * block, part)),
            pltpu.SemaphoreType.DMA((3,)),
            pltpu.SemaphoreType.DMA((HALVES,)),
            pltpu.SemaphoreType.DMA((HALVES,)),
            pltpu.SemaphoreType.DMA(((5 + PARTS) * HALVES,)),
        ],
        compiler_params=PARAMS,
        name="expert",
    )(recv, order, order_t, wg, wu, wd)


def combine_kernel(part, width, back, hits, masks, probs, input_grad, prob_grad, acc, pacc):
    step = pl.program_id(0)
    tops, tok = probs.shape
    last = width - (CHUNKS - 1) * part
    mark = -(-last // 128) * 128
    hit = hits[...]
    own = hit[:tok]
    for k in range(1, tops):
        own = own + hit[k * tok : (k + 1) * tok]
    mask = masks[...]
    spread = jnp.concatenate([own * mask[c : c + 1] for c in range(CHUNKS)], axis=0)
    blk = back[...]
    total = lax.dot_general(spread, blk, NN, preferred_element_type=F32)
    tails = hit * mask[CHUNKS - 1 : CHUNKS]
    tails = lax.dot_general(tails, blk[:, mark : mark + 128], NN, preferred_element_type=F32)

    @pl.when(step == 0)
    def _():
        acc[...] = total
        pacc[...] = tails

    @pl.when(step > 0)
    def _():
        acc[...] += total
        pacc[...] += tails

    @pl.when(step == pl.num_programs(0) - 1)
    def _():
        for c in range(CHUNKS):
            w = min(part, width - c * part)
            input_grad[c * part : c * part + w, :] = acc[c * tok : (c + 1) * tok, :].astype(BF).T[:w]
        for k in range(tops):
            col = pacc[k * tok : (k + 1) * tok, :].T
            prob_grad[k : k + 1, :] = (col[0:1] + col[1:2]) / probs[k : k + 1, :]


def combine(back, hits, masks, probs_t, width):
    rows, part = back.shape
    tops, tok = probs_t.shape
    span = masks.shape[1]
    turns = hits.shape[1] // span
    like = jax.ShapeDtypeStruct
    return pl.pallas_call(
        functools.partial(combine_kernel, part, width),
        grid=(rows // span,),
        out_shape=(like((width, tok), BF), like((tops, tok), F32)),
        in_specs=[
            pl.BlockSpec((span, part), lambda i: (i, 0)),
            pl.BlockSpec((tops * tok, span), lambda i: (0, i % turns)),
            pl.BlockSpec((CHUNKS, span), lambda i: (0, 0)),
            pl.BlockSpec((tops, tok), lambda i: (0, 0)),
        ],
        out_specs=(pl.BlockSpec((width, tok), lambda i: (0, 0)), pl.BlockSpec((tops, tok), lambda i: (0, 0))),
        scratch_shapes=[pltpu.VMEM((CHUNKS * tok, part), F32), pltpu.VMEM((tops * tok, 128), F32)],
        compiler_params=pltpu.CompilerParams(vmem_limit_bytes=24 * 1024 * 1024),
        name="combine",
    )(back, hits, masks, probs_t)

def divide(x, by):
    return jnp.floor((x.astype(F32) + 0.5) * (1.0 / by)).astype(jnp.int32)


def build_kernel(part, capacity, tokens_t, cotangent_t, ids, slots, probs, out, wide):
    width, tok = tokens_t.shape
    tops = ids.shape[0]
    position = jnp.where(slots[...] >= 0, ids[...] * capacity + slots[...], -1)

    @pl.when(pl.program_id(0) == 0)
    def _():
        for j, src in enumerate((tokens_t, cotangent_t)):
            for c in range(CHUNKS):
                w = min(part, width - c * part)
                wide[j, c * tok : (c + 1) * tok, :w] = src[c * part : c * part + w, :].T
                if w < part:
                    wide[j, c * tok : (c + 1) * tok, w:] = jnp.zeros((tok, part - w), BF)

    experts, both = out.shape[1:3]
    block = both // 2
    n = experts * block
    row = pl.program_id(0) * n + lax.broadcasted_iota(jnp.int32, (n, 1), 0)
    expert = divide(row, block)
    row = row - expert * block
    chunk = divide(row, capacity)
    slot = expert * capacity + row - chunk * capacity
    own = jnp.zeros((n, tok), F32)
    prob = jnp.zeros((n, tok), F32)
    for k in range(tops):
        hit = slot == position[k : k + 1, :]
        own = jnp.where(hit, 1.0, own)
        prob = jnp.where(hit, probs[k : k + 1, :], prob)
    pick = jnp.concatenate([jnp.where(chunk == c, own, 0.0).astype(BF) for c in range(CHUNKS)], axis=1)
    sent = lax.dot_general(pick, wide[0], NN, preferred_element_type=F32).astype(BF)
    cot = lax.dot_general(pick, wide[1], NN, preferred_element_type=F32)
    cot = (cot * jnp.sum(prob, axis=1, keepdims=True)).astype(BF)
    for d in range(out.shape[0]):
        out[d, :, :block, :] = sent.reshape(experts, block, part)
        out[d, :, block:, :] = cot.reshape(experts, block, part)


def build(tokens_t, cotangent_t, ids, slots, probs, capacity, experts, part, holders):
    width, tok = tokens_t.shape
    tops = ids.shape[0]
    both = 2 * CHUNKS * capacity
    steps = STEPS
    whole = lambda shape: pl.BlockSpec(shape, lambda i: (0,) * len(shape))
    return pl.pallas_call(
        functools.partial(build_kernel, part, capacity),
        grid=(steps,),
        out_shape=jax.ShapeDtypeStruct((holders, experts, both, part), BF),
        in_specs=[whole((width, tok))] * 2 + [whole((tops, tok))] * 3,
        out_specs=pl.BlockSpec((holders, experts // steps, both, part), lambda i: (0, i, 0, 0)),
        scratch_shapes=[pltpu.VMEM((2, CHUNKS * tok, part), BF)],
        compiler_params=PARAMS,
        name="build",
    )(tokens_t, cotangent_t, ids, slots, probs)


def body(tokens, cotangent, expert_ids, slots, probs, w_gate, w_up, w_down):
    experts = lax.axis_size("expert")
    holders = lax.axis_size("dp")
    tok_rows, width = tokens.shape
    top_count = expert_ids.shape[1]
    capacity = max(2, 3 * tok_rows * top_count // (4 * experts))
    part = -(-width // (CHUNKS * 128)) * 128
    devices = holders * experts
    block = CHUNKS * capacity
    send_rows = experts * block
    position = jnp.where(slots >= 0, expert_ids * capacity + slots, -1).T
    probs_t = probs.T

    row = jnp.arange(send_rows, dtype=jnp.int32)
    row_slot = (row // block) * capacity + row % capacity
    row_chunk = (row // capacity) % CHUNKS

    i = np.arange(GROUP * block)
    source, chunk, slot = (i // capacity) % GROUP, i // (GROUP * capacity), i % capacity
    target = source * block + chunk * capacity + slot
    order = jnp.asarray(target[:, None] == i[None, :], BF)
    order_t = jnp.asarray(i[:, None] == target[None, :], BF)

    def exchange(blocks):
        return lax.all_to_all(blocks, ("dp", "expert"), split_axis=0, concat_axis=0, tiled=True)

    gate_w = w_gate[0].T
    up_w = w_up[0].T
    down_w = w_down[0].T
    sent = build(tokens.T, cotangent.T, expert_ids.T, slots.T, probs_t, capacity, experts, part, holders)
    recv = exchange(sent.reshape(devices, 2 * block, part))
    hits = (position.reshape(top_count * tok_rows, 1) == row_slot[None, :]).astype(BF)
    masks = (row_chunk[None, : send_rows // TURNS] == jnp.arange(CHUNKS)[:, None]).astype(BF)
    ret, rows, weighted, hidden, gate_grad, up_grad = expert(recv, order, order_t, gate_w, up_w, down_w)
    back = exchange(ret.reshape(devices, block, part)).reshape(devices * block, part)
    with jax.named_scope("weight_grads"):
        grad_down = lax.dot_general(weighted, hidden, TN, preferred_element_type=F32).astype(BF)
        grad_gate = lax.dot_general(rows, gate_grad, TN, preferred_element_type=F32).astype(BF)
        grad_up = lax.dot_general(rows, up_grad, TN, preferred_element_type=F32).astype(BF)
    with jax.named_scope("combine"):
        input_grad, prob_grad = combine(back, hits, masks, probs_t, width)
    return (input_grad.T, prob_grad.T, grad_gate[None], grad_up[None], grad_down[None])


def solution(mesh):
    tokens = P(("expert", "dp"), None)
    weights = P("expert", None, "dp")
    return jax.shard_map(
        body,
        mesh=mesh,
        in_specs=(tokens,) * 5 + (weights,) * 3,
        out_specs=(tokens,) * 2 + (weights,) * 3,
        check_vma=False,
    )
```

```python
import functools

import jax
import jax.numpy as jnp
import numpy as np
from jax import lax
from jax.experimental import pallas as pl
from jax.experimental.pallas import tpu as pltpu
from jax.sharding import PartitionSpec as P

ALPHA = 1.702
CHUNKS = 4
GROUP = 8
HALVES = 2
PARTS = 2
UNROLL = 8
STEPS = 4
TURNS = 1
BF = jnp.bfloat16
F32 = jnp.float32
NT = (((1,), (1,)), ((), ()))
NN = (((1,), (0,)), ((), ()))
TN = (((0,), (0,)), ((), ()))
ANY = pl.BlockSpec(memory_space=pl.ANY)
VMEM = pl.BlockSpec(memory_space=pltpu.VMEM)
PARAMS = pltpu.CompilerParams(vmem_limit_bytes=60 * 1024 * 1024)


def sort_rows(recv, pick, out, i, part, width):
    size = pick.shape[0]
    lane_rows = size // CHUNKS
    groups = recv.shape[0] // GROUP

    def step(b, carry):
        blk = recv[pl.ds(b * GROUP, GROUP)].reshape(size, part)
        picked = lax.dot_general(pick, blk, NN, preferred_element_type=F32).astype(BF)
        at = pl.ds(pl.multiple_of(b * lane_rows, lane_rows), lane_rows)
        for c in range(CHUNKS):
            w = min(part, width - c * part)
            out[at, c * part : c * part + w] = picked[c * lane_rows : (c + 1) * lane_rows, :w]
        return carry

    lax.fori_loop(i * groups // HALVES, (i + 1) * groups // HALVES, step, 0, unroll=UNROLL)


def expert_kernel(
    part, recv_hbm, order, order_t, wg_hbm, wu_hbm, wd_hbm,
    ret_hbm, rows_hbm, weighted_hbm, hidden_hbm, gate_hbm, up_hbm,
    recv_t, recv_c, wg, wu, wd, rows, weighted, hidden, glu, slope, gate_grad, up_grad, wide, ret,
    in_sems, t_sems, c_sems, out_sems,
):
    units, width = wg.shape
    total = rows.shape[0]
    m = total // HALVES
    last = width - (CHUNKS - 1) * part
    mark = -(-last // 128) * 128
    size = order.shape[0]
    lane_rows = size // CHUNKS
    block = recv_t.shape[1]
    sources = recv_t.shape[0]
    span = sources // HALVES

    def pieces(dst, first, sems):
        return [
            pltpu.make_async_copy(
                recv_hbm.at[pl.ds(p * span, span), pl.ds(first, block)], dst.at[pl.ds(p * span, span)], sems.at[p]
            )
            for p in range(HALVES)
        ]

    def load(src, dst, i):
        return pltpu.make_async_copy(src, dst, in_sems.at[i])

    stores = []

    def store(src, dst):
        stores.append(pltpu.make_async_copy(src, dst, out_sems.at[len(stores)]))
        stores[-1].start()

    t_loads = pieces(recv_t, 0, t_sems)
    c_loads = pieces(recv_c, block, c_sems)
    g_load, u_load, d_load = load(wg_hbm, wg, 0), load(wu_hbm, wu, 1), load(wd_hbm, wd, 2)
    for copy in (t_loads[0], g_load, u_load, *t_loads[1:], d_load, *c_loads):
        copy.start()
    pick = order[...]
    pick_t = order_t[...]
    for i in range(HALVES):
        at = pl.ds(i * m, m)
        t_loads[i].wait()
        sort_rows(recv_t, pick, rows, i, part, width)
        store(rows.at[at], rows_hbm.at[at])
        if i == 0:
            g_load.wait()
        g = lax.dot_general(rows[at, :], wg[...], NT, preferred_element_type=F32)
        if i == 0:
            u_load.wait()
        u = lax.dot_general(rows[at, :], wu[...], NT, preferred_element_type=F32) + 1.0
        s = jax.nn.sigmoid(ALPHA * g)
        gl = g * s
        hidden[at, :] = (u * gl).astype(BF)
        glu[at, :] = gl
        slope[at, :] = u * (s + ALPHA * g * s * (1.0 - s))
        store(hidden.at[at], hidden_hbm.at[at])
    for i in range(HALVES):
        at = pl.ds(i * m, m)
        c_loads[i].wait()
        sort_rows(recv_c, pick, weighted, i, part, width)
        store(weighted.at[at], weighted_hbm.at[at])
        if i == 0:
            d_load.wait()
        hg = lax.dot_general(weighted[at, :], wd[...], NT, preferred_element_type=F32)
        sg = jnp.sum(hg * hidden[at, :].astype(F32), axis=1, keepdims=True)
        ug = (hg * glu[at, :]).astype(BF)
        gg = (hg * slope[at, :]).astype(BF)
        gate_grad[at, :] = gg
        up_grad[at, :] = ug
        store(gate_grad.at[at], gate_hbm.at[at])
        store(up_grad.at[at], up_hbm.at[at])
        low = sg - sg.astype(BF).astype(F32)
        lane = lax.broadcasted_iota(jnp.int32, (m, part - mark), 1)
        tail = jnp.where(lane == 0, sg, jnp.where(lane == 1, low, 0.0)).astype(BF)
        if last < mark:
            wide[CHUNKS - 1, :, mark - 128 : mark] = jnp.zeros((m, 128), BF)
        wide[CHUNKS - 1, :, mark:] = tail
        for c in range(CHUNKS):
            w = min(part, width - c * part)
            x = lax.dot_general(gg, wg[:, c * part : c * part + w], NN, preferred_element_type=F32)
            x = x + lax.dot_general(ug, wu[:, c * part : c * part + w], NN, preferred_element_type=F32)
            wide[c, :, :w] = x.astype(BF)
        first = i * (ret.shape[0] // HALVES)

        def put(b, carry):
            src = pl.ds(pl.multiple_of(b * lane_rows, lane_rows), lane_rows)
            blk = jnp.concatenate([wide[c, src, :] for c in range(CHUNKS)], axis=0)
            out = lax.dot_general(pick_t, blk, NN, preferred_element_type=F32)
            ret[pl.ds(pl.multiple_of(first + b * size, size), size), :] = out.astype(BF)
            return carry

        turns = m // lane_rows // PARTS
        for q in range(PARTS):
            lax.fori_loop(q * turns, (q + 1) * turns, put, 0, unroll=2)
            done = pl.ds(first + q * turns * size, turns * size)
            store(ret.at[done], ret_hbm.at[done])
    for copy in stores:
        copy.wait()


def expert(recv, order, order_t, wg, wu, wd):
    units, width = wg.shape
    sources, both, part = recv.shape
    block = both // 2
    total = sources * block // CHUNKS
    like = jax.ShapeDtypeStruct
    scratch = lambda shape, dtype=BF: pltpu.VMEM(shape, dtype)
    return pl.pallas_call(
        functools.partial(expert_kernel, part),
        out_shape=(
            like((sources * block, part), BF),
            like((total, width), BF),
            like((total, width), BF),
            like((total, units), BF),
            like((total, units), BF),
            like((total, units), BF),
        ),
        in_specs=[ANY, VMEM, VMEM, ANY, ANY, ANY],
        out_specs=(ANY,) * 6,
        scratch_shapes=[
            scratch((sources, block, part)),
            scratch((sources, block, part)),
            scratch((units, width)),
            scratch((units, width)),
            scratch((units, width)),
            scratch((total, width)),
            scratch((total, width)),
            scratch((total, units)),
            scratch((total, units), F32),
            scratch((total, units), F32),
            scratch((total, units)),
            scratch((total, units)),
            scratch((CHUNKS, total // HALVES, part)),
            scratch((sources * block, part)),
            pltpu.SemaphoreType.DMA((3,)),
            pltpu.SemaphoreType.DMA((HALVES,)),
            pltpu.SemaphoreType.DMA((HALVES,)),
            pltpu.SemaphoreType.DMA(((5 + PARTS) * HALVES,)),
        ],
        compiler_params=PARAMS,
        name="expert",
    )(recv, order, order_t, wg, wu, wd)


def combine_kernel(part, width, back, hits, masks, probs, input_grad, prob_grad, acc, pacc):
    step = pl.program_id(0)
    tops, tok = probs.shape
    last = width - (CHUNKS - 1) * part
    mark = -(-last // 128) * 128
    hit = hits[...]
    own = hit[:tok]
    for k in range(1, tops):
        own = own + hit[k * tok : (k + 1) * tok]
    mask = masks[...]
    spread = jnp.concatenate([own * mask[c : c + 1] for c in range(CHUNKS)], axis=0)
    blk = back[...]
    total = lax.dot_general(spread, blk, NN, preferred_element_type=F32)
    tails = hit * mask[CHUNKS - 1 : CHUNKS]
    tails = lax.dot_general(tails, blk[:, mark : mark + 128], NN, preferred_element_type=F32)

    @pl.when(step == 0)
    def _():
        acc[...] = total
        pacc[...] = tails

    @pl.when(step > 0)
    def _():
        acc[...] += total
        pacc[...] += tails

    @pl.when(step == pl.num_programs(0) - 1)
    def _():
        for c in range(CHUNKS):
            w = min(part, width - c * part)
            input_grad[c * part : c * part + w, :] = acc[c * tok : (c + 1) * tok, :].astype(BF).T[:w]
        for k in range(tops):
            col = pacc[k * tok : (k + 1) * tok, :].T
            prob_grad[k : k + 1, :] = (col[0:1] + col[1:2]) / probs[k : k + 1, :]


def combine(back, hits, masks, probs_t, width):
    rows, part = back.shape
    tops, tok = probs_t.shape
    span = masks.shape[1]
    turns = hits.shape[1] // span
    like = jax.ShapeDtypeStruct
    return pl.pallas_call(
        functools.partial(combine_kernel, part, width),
        grid=(rows // span,),
        out_shape=(like((width, tok), BF), like((tops, tok), F32)),
        in_specs=[
            pl.BlockSpec((span, part), lambda i: (i, 0)),
            pl.BlockSpec((tops * tok, span), lambda i: (0, i % turns)),
            pl.BlockSpec((CHUNKS, span), lambda i: (0, 0)),
            pl.BlockSpec((tops, tok), lambda i: (0, 0)),
        ],
        out_specs=(pl.BlockSpec((width, tok), lambda i: (0, 0)), pl.BlockSpec((tops, tok), lambda i: (0, 0))),
        scratch_shapes=[pltpu.VMEM((CHUNKS * tok, part), F32), pltpu.VMEM((tops * tok, 128), F32)],
        compiler_params=pltpu.CompilerParams(vmem_limit_bytes=24 * 1024 * 1024),
        name="combine",
    )(back, hits, masks, probs_t)

def divide(x, by):
    return jnp.floor((x.astype(F32) + 0.5) * (1.0 / by)).astype(jnp.int32)


def build_kernel(part, capacity, tokens_t, cotangent_t, ids, slots, probs, out, wide):
    width, tok = tokens_t.shape
    tops = ids.shape[0]
    position = jnp.where(slots[...] >= 0, ids[...] * capacity + slots[...], -1)

    @pl.when(pl.program_id(0) == 0)
    def _():
        for j, src in enumerate((tokens_t, cotangent_t)):
            for c in range(CHUNKS):
                w = min(part, width - c * part)
                wide[j, c * tok : (c + 1) * tok, :w] = src[c * part : c * part + w, :].T
                if w < part:
                    wide[j, c * tok : (c + 1) * tok, w:] = jnp.zeros((tok, part - w), BF)

    experts, both = out.shape[1:3]
    block = both // 2
    n = experts * block
    row = pl.program_id(0) * n + lax.broadcasted_iota(jnp.int32, (n, 1), 0)
    expert = divide(row, block)
    row = row - expert * block
    chunk = divide(row, capacity)
    slot = expert * capacity + row - chunk * capacity
    own = jnp.zeros((n, tok), F32)
    prob = jnp.zeros((n, tok), F32)
    for k in range(tops):
        hit = slot == position[k : k + 1, :]
        own = jnp.where(hit, 1.0, own)
        prob = jnp.where(hit, probs[k : k + 1, :], prob)
    pick = jnp.concatenate([jnp.where(chunk == c, own, 0.0).astype(BF) for c in range(CHUNKS)], axis=1)
    sent = lax.dot_general(pick, wide[0], NN, preferred_element_type=F32).astype(BF)
    cot = lax.dot_general(pick, wide[1], NN, preferred_element_type=F32)
    cot = (cot * jnp.sum(prob, axis=1, keepdims=True)).astype(BF)
    for d in range(out.shape[0]):
        out[d, :, :block, :] = sent.reshape(experts, block, part)
        out[d, :, block:, :] = cot.reshape(experts, block, part)


def build(tokens_t, cotangent_t, ids, slots, probs, capacity, experts, part, holders):
    width, tok = tokens_t.shape
    tops = ids.shape[0]
    both = 2 * CHUNKS * capacity
    steps = STEPS
    whole = lambda shape: pl.BlockSpec(shape, lambda i: (0,) * len(shape))
    return pl.pallas_call(
        functools.partial(build_kernel, part, capacity),
        grid=(steps,),
        out_shape=jax.ShapeDtypeStruct((holders, experts, both, part), BF),
        in_specs=[whole((width, tok))] * 2 + [whole((tops, tok))] * 3,
        out_specs=pl.BlockSpec((holders, experts // steps, both, part), lambda i: (0, i, 0, 0)),
        scratch_shapes=[pltpu.VMEM((2, CHUNKS * tok, part), BF)],
        compiler_params=PARAMS,
        name="build",
    )(tokens_t, cotangent_t, ids, slots, probs)


def body(tokens, cotangent, expert_ids, slots, probs, w_gate, w_up, w_down):
    experts = lax.axis_size("expert")
    holders = lax.axis_size("dp")
    tok_rows, width = tokens.shape
    top_count = expert_ids.shape[1]
    capacity = max(2, 3 * tok_rows * top_count // (4 * experts))
    part = -(-width // (CHUNKS * 128)) * 128
    devices = holders * experts
    block = CHUNKS * capacity
    send_rows = experts * block
    position = jnp.where(slots >= 0, expert_ids * capacity + slots, -1).T
    probs_t = probs.T

    row = jnp.arange(send_rows, dtype=jnp.int32)
    row_slot = (row // block) * capacity + row % capacity
    row_chunk = (row // capacity) % CHUNKS

    i = np.arange(GROUP * block)
    source, chunk, slot = (i // capacity) % GROUP, i // (GROUP * capacity), i % capacity
    target = source * block + chunk * capacity + slot
    order = jnp.asarray(target[:, None] == i[None, :], BF)
    order_t = jnp.asarray(i[:, None] == target[None, :], BF)

    def exchange(blocks):
        return lax.all_to_all(blocks, ("dp", "expert"), split_axis=0, concat_axis=0, tiled=True)

    gate_w = w_gate[0].T
    up_w = w_up[0].T
    down_w = w_down[0].T
    sent = build(tokens.T, cotangent.T, expert_ids.T, slots.T, probs_t, capacity, experts, part, holders)
    recv = exchange(sent.reshape(devices, 2 * block, part))
    hits = (position.reshape(top_count * tok_rows, 1) == row_slot[None, :]).astype(BF)
    masks = (row_chunk[None, : send_rows // TURNS] == jnp.arange(CHUNKS)[:, None]).astype(BF)
    ret, rows, weighted, hidden, gate_grad, up_grad = expert(recv, order, order_t, gate_w, up_w, down_w)
    back = exchange(ret.reshape(devices, block, part)).reshape(devices * block, part)
    with jax.named_scope("weight_grads"):
        grad_down = lax.dot_general(weighted, hidden, TN, preferred_element_type=F32).astype(BF)
        grad_gate = lax.dot_general(rows, gate_grad, TN, preferred_element_type=F32).astype(BF)
        grad_up = lax.dot_general(rows, up_grad, TN, preferred_element_type=F32).astype(BF)
    with jax.named_scope("combine"):
        input_grad, prob_grad = combine(back, hits, masks, probs_t, width)
    return (input_grad.T, prob_grad.T, grad_gate[None], grad_up[None], grad_down[None])


def solution(mesh):
    tokens = P(("expert", "dp"), None)
    weights = P("expert", None, "dp")
    return jax.shard_map(
        body,
        mesh=mesh,
        in_specs=(tokens,) * 5 + (weights,) * 3,
        out_specs=(tokens,) * 2 + (weights,) * 3,
        check_vma=False,
    )
```
